32 devices in a mesh: grp: 8 (over y, x, core), rep: 4 (over z).
Axes of the slice: x: 2, y: 2, z: 4, core: 2. Of those that a mesh axis runs over, the one named last changes fastest.
Arguments:
- momentum: bfloat16 [256, 4096], P(('grp', 'rep')), may hold values from -6 to 6
- picked: int32 [256, 32], P(('grp', 'rep')), may hold values from 0 to 4095, as said below
- owner_span_order: int32 [8], replicated, may hold values from 0 to 7, each once
Outputs:
- update: bfloat16 [8, 4096], replicated
- residual_momentum: bfloat16 [256, 4096], P(('grp', 'rep'))
The draws below stay inside these ranges and needn't reach their ends.
Inputs may be any that keep to these rules, and one draw needn't show every extreme that they name: `picked`: the 32 numbers of a row are different. `owner_span_order`: each span stands once.
All inputs are finite; a program needn't handle non-finite values.
Results may differ from the reference program's by a relative error of at most 0.013.
Values may be sent and summed in bfloat16 or wider, within the bound.
A program may use at most 64 MiB of HBM per device.

```python
import jax
import jax.numpy as jnp
from jax import lax

BLOCK = 64
COMP = 4096
TOPK = 32
SPANS = 8
DEVICES = 32


def draw_picked(key, part):
    streams = jax.random.split(jax.random.fold_in(key, 11), DEVICES)

    def one_device(stream):
        scores = jax.random.randint(stream, (SPANS, COMP), 0, 2 ** 18, dtype=jnp.int32) * COMP
        scores = scores + jnp.arange(COMP, dtype=jnp.int32)[None, :]
        return lax.top_k(scores, TOPK)[1].astype(jnp.int32)
    return lax.map(one_device, streams).reshape(DEVICES * SPANS, TOPK)


def block_scale(rng, extent, cuts, smallest, high):
    def one(position, blocks):
        draws = jax.random.uniform(jax.random.fold_in(jax.random.fold_in(rng, 6), position), (blocks,), jnp.float32, smallest / len(cuts), high / len(cuts))
        return jnp.repeat(jnp.exp(draws), extent[position] // blocks).reshape((-1,) + (1,) * (len(extent) - position - 1))

    gain = one(*cuts[0])
    for cut in cuts[1:]:
        gain = gain * one(*cut)
    return gain


def scatter_about(stream_key, shape, scale, limit, pieces=(), kind=jnp.bfloat16):
    drawn = jax.random.normal(stream_key, shape, jnp.float32) * scale
    if len(pieces) > 0:
        drawn = block_scale(stream_key, shape, pieces, -0.22, 0.18) * drawn
    return jnp.clip(drawn, min=-limit, max=limit).astype(kind)


def setup_inputs(seed: int = 0) -> dict:
    seeds = jax.random.split(jax.random.key(seed), 4)
    return {
        "momentum": scatter_about(seeds[0], (DEVICES * SPANS, COMP), 1.0, 6.0, ((0, 32),)),
        "picked": draw_picked(jax.random.fold_in(seeds[3], 71), 0),
        "owner_span_order": jax.random.permutation(seeds[2], SPANS).astype(jnp.int32),
    }


def dct_cosines(points):
    freq = jnp.arange(points, dtype=jnp.float32)[:, None]
    place = jnp.arange(points, dtype=jnp.float32)[None, :]
    values = jnp.cos(jnp.pi * (2.0 * place + 1.0) * freq / (2.0 * points)) * jnp.sqrt(2.0 / points)
    values = values.at[0].multiply(jnp.sqrt(0.5))
    rounded = lax.optimization_barrier(values.astype(jnp.bfloat16))
    return rounded.astype(jnp.float32)

def decode(dense_matrix, cosines):
    square = dense_matrix.reshape(dense_matrix.shape[0], BLOCK, BLOCK)
    half = jnp.einsum('cij,jb->cib', square, cosines, precision=lax.Precision.HIGHEST)
    full = jnp.einsum('ia,cib->cab', cosines, half, precision=lax.Precision.HIGHEST)
    return full.reshape(dense_matrix.shape[0], COMP)

def reference(momentum, picked, owner_span_order):
    cosines = dct_cosines(BLOCK)
    incoming_blocks = momentum.reshape(DEVICES, SPANS, COMP)
    picks = picked.reshape(DEVICES, SPANS, TOPK)
    span_rows = jnp.broadcast_to(jnp.arange(SPANS, dtype=jnp.int32)[:, None], (SPANS, TOPK))

    def accumulate_into(summed, input_list):
        momentum_dev, picks_dev = input_list
        square = momentum_dev.astype(jnp.float32).reshape(SPANS, BLOCK, BLOCK)
        half = jnp.einsum('cab,jb->caj', square, cosines, precision=lax.Precision.HIGHEST)
        freq_rows = cosines[picks_dev // BLOCK]
        freq_cols = cosines[picks_dev % BLOCK]
        half_cols = jnp.take_along_axis(half, (picks_dev % BLOCK)[:, None, :], axis=2)
        coeff_vals = jnp.einsum('cta,cat->ct', freq_rows, half_cols, precision=lax.Precision.HIGHEST)
        chosen = coeff_vals.astype(jnp.bfloat16).astype(jnp.float32)
        correction = jnp.einsum('cta,ctb->cab', freq_rows * chosen[:, :, None], freq_cols, precision=lax.Precision.HIGHEST)
        residual = (momentum_dev.astype(jnp.float32) - correction.reshape(SPANS, COMP)).astype(jnp.bfloat16)
        summed = summed.at[span_rows, picks_dev].add(chosen)
        return (summed, residual)
    summed, residuals = lax.scan(accumulate_into, jnp.zeros((SPANS, COMP), jnp.float32), (incoming_blocks, picks))
    decoded = decode(summed, cosines)
    update = decoded[owner_span_order].astype(jnp.bfloat16)
    return (update, residuals.reshape(DEVICES * SPANS, COMP))
```

```python
import math

import functools

import jax
import jax.numpy as jnp
import numpy as np
from jax import lax
from jax.experimental import pallas as pl
from jax.experimental.pallas import tpu as pltpu
from jax.sharding import PartitionSpec as P

BLOCK = 64
TOPK = 32
CH_OWN = 1


def dct_cosines(points):
    freq = jnp.arange(points, dtype=jnp.float32)[:, None]
    place = jnp.arange(points, dtype=jnp.float32)[None, :]
    values = jnp.cos(jnp.pi * (2.0 * place + 1.0) * freq / (2.0 * points)) * jnp.sqrt(2.0 / points)
    values = values.at[0].multiply(jnp.sqrt(0.5))
    rounded = lax.optimization_barrier(values.astype(jnp.bfloat16))
    return rounded.astype(jnp.float32)


def forward(square_low, cosines, cos_low):
    half = jnp.einsum("cab,jb->caj", square_low, cos_low, preferred_element_type=jnp.float32)
    return jnp.einsum("ia,caj->cij", cosines, half, precision=lax.Precision.HIGHEST)


def decode(dense_matrix, cosines):
    square = dense_matrix.reshape(dense_matrix.shape[0], BLOCK, BLOCK)
    half = jnp.einsum("cij,jb->cib", square, cosines, precision=lax.Precision.HIGHEST)
    full = jnp.einsum("ia,cib->cab", cosines, half, precision=lax.Precision.HIGHEST)
    return full.reshape(dense_matrix.shape[0], BLOCK * BLOCK)


def decode_sparse(dense_low, cosines, cos_low):
    square = dense_low.reshape(dense_low.shape[0], BLOCK, BLOCK)
    half = jnp.einsum("cij,jb->cib", square, cos_low, preferred_element_type=jnp.float32)
    full = jnp.einsum("ia,cib->cab", cosines, half, precision=lax.Precision.HIGHEST)
    return full.reshape(dense_low.shape[0], BLOCK * BLOCK)


def densify(values, spots):
    entries, columns = values.shape
    per_step = math.gcd(entries, max(1, 65536 // columns))
    positions = jnp.arange(BLOCK, dtype=jnp.int32)

    def one_block(pieces):
        block_values, block_spots = pieces
        zeros = jnp.zeros_like(block_values)
        row_onehot = jnp.where(
            (block_spots // BLOCK)[:, None, :] == positions[None, :, None],
            block_values[:, None, :],
            zeros[:, None, :],
        )
        column_onehot = ((block_spots % BLOCK)[:, None, :] == positions[None, :, None]).astype(
            jnp.bfloat16
        )
        dense_matrix = jnp.einsum(
            "bcy,bzy->bcz", row_onehot, column_onehot, preferred_element_type=jnp.float32
        )
        return dense_matrix.reshape(per_step, BLOCK * BLOCK)

    stacked = lax.map(
        one_block,
        (
            values.reshape(entries // per_step, per_step, columns),
            spots.reshape(entries // per_step, per_step, columns),
        ),
    )
    return stacked.reshape(entries, BLOCK * BLOCK)


def owner_sum(received):
    values, spots = received
    return densify(values[0], spots[0])


def local_large(momentum, picked, owner_span_order):
    cosines = dct_cosines(BLOCK)
    cos_low = cosines.astype(jnp.bfloat16)
    owners = lax.axis_size("grp")
    span_count = momentum.shape[0]
    square_low = momentum.reshape(span_count, BLOCK, BLOCK)
    transform_coefficients = forward(square_low, cosines, cos_low).reshape(
        span_count, BLOCK * BLOCK
    )
    chosen = jnp.take_along_axis(transform_coefficients, picked, axis=1).astype(jnp.bfloat16)
    own_dense = densify(chosen, picked).astype(jnp.bfloat16)
    residual_momentum = (
        momentum.astype(jnp.float32) - decode_sparse(own_dense, cosines, cos_low)
    ).astype(jnp.bfloat16)
    slot_values = jnp.take(chosen, owner_span_order, axis=0)
    slot_spots = jnp.take(picked, owner_span_order, axis=0)
    shaped = (slot_values.reshape(owners, CH_OWN, TOPK), slot_spots.reshape(owners, CH_OWN, TOPK))
    partial_sum = owner_sum(
        (
            lax.all_to_all(shaped[0], "grp", split_axis=0, concat_axis=2, tiled=True),
            lax.all_to_all(shaped[1], "grp", split_axis=0, concat_axis=2, tiled=True),
        )
    )
    partial_sum = lax.psum(partial_sum, "rep")
    my_share = decode(partial_sum, cosines).astype(jnp.bfloat16)
    update = lax.all_gather(my_share, "grp", axis=0, tiled=True)
    return (update, residual_momentum)


LANES = 128
GATHER_BYTES = 2**20


def cosine_table():
    freq = np.arange(BLOCK, dtype=np.float64)[:, None]
    place = np.arange(BLOCK, dtype=np.float64)[None, :]
    values = np.cos(np.pi * (2 * place + 1) * freq / (2 * BLOCK)) * np.sqrt(2 / BLOCK)
    values[0] *= np.sqrt(0.5)
    return values.astype(np.float32)


def contract_lanes(left, right):
    return lax.dot_general(
        left, right, (((1,), (1,)), ((), ())), preferred_element_type=jnp.float32
    )


def matmul(left, right):
    return jnp.dot(left, right, preferred_element_type=jnp.float32)


def split(value):
    high = value.astype(jnp.bfloat16)
    return high, (value - high.astype(jnp.float32)).astype(jnp.bfloat16)


def exchange_kernel(
    groups,
    planes,
    order_ref,
    momentum_ref,
    picked_ref,
    rows_ref,
    cols_ref,
    twice_ref,
    pairs_ref,
    update_ref,
    residual_ref,
    box,
    dense,
    decoded,
    send_sem,
    recv_sem,
):
    spans = momentum_ref.shape[0]
    entries = spans * TOPK
    chunks = BLOCK * BLOCK // LANES
    in_tile = LANES // TOPK
    tiles = entries // LANES
    devices = groups * planes
    my_group, my_plane = lax.axis_index("grp"), lax.axis_index("rep")
    group_of = [lax.rem(my_group + step, groups) for step in range(groups)]
    plane_of = [lax.rem(my_plane + step, planes) for step in range(planes)]

    def peer(plane, group):
        return {"grp": group_of[group], "rep": plane_of[plane]}

    others = [(z, g) for z in range(planes) for g in range(groups) if z or g]
    barrier = pltpu.get_barrier_semaphore()
    for z, g in others[::-1]:
        pl.semaphore_signal(barrier, inc=1, device_id=peer(z, g), device_id_type=pl.DeviceIdType.MESH)

    lane = lax.broadcasted_iota(jnp.int32, (spans, entries), 1)
    mine = (lane // TOPK) == lax.broadcasted_iota(jnp.int32, (spans, entries), 0)
    spread = jnp.concatenate([picked_ref[...]] * spans, axis=1)
    spots = jnp.sum(jnp.where(mine, spread, 0), axis=0, keepdims=True)
    freq = lax.broadcasted_iota(jnp.int32, (BLOCK, entries), 0)
    one_row = jnp.where(freq == spots // BLOCK, 1.0, 0.0).astype(jnp.bfloat16)
    one_col = jnp.where(freq == spots % BLOCK, 1.0, 0.0).astype(jnp.bfloat16)
    half_rows = chunks * spans
    wave = matmul(cols_ref[...], one_col).astype(jnp.bfloat16)
    blank = jnp.zeros_like(wave)
    waves = (jnp.concatenate([wave, blank], axis=0), jnp.concatenate([blank, wave], axis=0))
    momentum = jnp.concatenate(
        [momentum_ref[:, k * LANES : (k + 1) * LANES].astype(jnp.float32) for k in range(chunks)],
        axis=0,
    )
    momentum_low = momentum.astype(jnp.bfloat16)
    total = jnp.zeros((spans, entries), jnp.float32)
    row_waves = []
    for p in range(2):
        row_wave = matmul(rows_ref[p * half_rows : (p + 1) * half_rows, :], one_row)
        row_waves.append(row_wave)
        product = row_wave * matmul(momentum_low, waves[p])
        total += jnp.sum(product.reshape(chunks, spans, entries), axis=0)
    chosen = jnp.sum(jnp.where(mine, total, 0.0), axis=0, keepdims=True)
    chosen = chosen.astype(jnp.bfloat16).astype(jnp.float32)
    box[0, 0:1, :] = chosen
    box[0, 1:2, :] = spots.astype(jnp.float32)

    pl.semaphore_wait(barrier, devices - 1)
    copies = []
    for z, g in others[::-1]:
        copy = pltpu.make_async_remote_copy(
            src_ref=box.at[0],
            dst_ref=box.at[z * groups + g],
            send_sem=send_sem,
            recv_sem=recv_sem.at[z],
            device_id=peer(z, g),
            device_id_type=pl.DeviceIdType.MESH,
        )
        copy.start()
        copies.append(copy)

    correction = jnp.zeros((half_rows, LANES), jnp.float32)
    scaled = jnp.where(mine, chosen, 0.0)
    for p in range(2):
        weight = row_waves[p].reshape(chunks, spans, entries) * scaled[None]
        for part in split(weight.reshape(half_rows, entries)):
            correction += contract_lanes(part, waves[p])
    residual = momentum - correction
    for k in range(chunks):
        residual_ref[:, k * LANES : (k + 1) * LANES] = residual[
            k * spans : (k + 1) * spans
        ].astype(jnp.bfloat16)

    offset = (lax.broadcasted_iota(jnp.int32, (1, LANES), 1) // TOPK) * BLOCK
    tall = lax.broadcasted_iota(jnp.int32, (in_tile * BLOCK, LANES), 0)
    short = lax.broadcasted_iota(jnp.int32, (BLOCK, LANES), 0)
    sums = [jnp.zeros((in_tile * BLOCK, BLOCK), jnp.float32) for _ in range(tiles)]
    reach = sorted(range(planes), key=lambda z: min(z, planes - z))
    for z in reach:
        first = 1 if z == 0 else 0
        landed = box.at[pl.ds(z * groups + first, groups - first)]
        pltpu.make_async_copy(landed, landed, recv_sem.at[z]).wait()
        for h in range(tiles):
            left, right = [], []
            for g in range(groups):
                slot = box[z * groups + g, :, h * LANES : (h + 1) * LANES]
                value = slot[0:1]
                spot = slot[1:2].astype(jnp.int32)
                left.append(jnp.where(tall == spot // BLOCK + offset, 1.0, 0.0).astype(jnp.bfloat16))
                right.append(jnp.where(short == spot % BLOCK, value, 0.0).astype(jnp.bfloat16))
            sums[h] += contract_lanes(
                jnp.concatenate(left, axis=1), jnp.concatenate(right, axis=1)
            )
    lower = lax.broadcasted_iota(jnp.int32, (BLOCK, LANES), 1) < BLOCK
    for h in range(tiles):
        half = sum(matmul(part, twice_ref[...]) for part in split(sums[h]))
        for c in range(in_tile):
            dense[h * in_tile + c] = half[c * BLOCK : (c + 1) * BLOCK]
    for s in range(spans):
        half = dense[order_ref[s]]
        stacked = jnp.concatenate(
            [jnp.where(lower, half, 0.0), jnp.where(lower, 0.0, half)], axis=0
        )
        decoded[pl.ds(s, chunks, stride=spans), :] = matmul(
            pairs_ref[...], stacked.astype(jnp.bfloat16)
        )
    for k in range(chunks):
        update_ref[:, k * LANES : (k + 1) * LANES] = decoded[
            k * spans : (k + 1) * spans, :
        ].astype(jnp.bfloat16)
    for copy in copies:
        copy.wait_send()


def local_small(groups, planes, momentum, picked, owner_span_order):
    spans = momentum.shape[0]
    chunks = BLOCK * BLOCK // LANES
    table = cosine_table()
    by_pair = table.T.reshape(chunks, 2, BLOCK)
    rows = np.repeat(by_pair.transpose(1, 0, 2), spans, axis=1).reshape(-1, BLOCK)
    constants = [rows, table.T, np.concatenate([table, table], axis=1), by_pair.reshape(chunks, LANES)]
    vmem = pl.BlockSpec(memory_space=pltpu.VMEM)
    return pl.pallas_call(
        functools.partial(exchange_kernel, groups, planes),
        out_shape=(
            jax.ShapeDtypeStruct(momentum.shape, jnp.bfloat16),
            jax.ShapeDtypeStruct(momentum.shape, jnp.bfloat16),
        ),
        in_specs=[pl.BlockSpec(memory_space=pltpu.SMEM)] + [vmem] * 6,
        out_specs=(vmem, vmem),
        scratch_shapes=[
            pltpu.VMEM((groups * planes, 2, spans * TOPK), jnp.float32),
            pltpu.VMEM((spans, BLOCK, LANES), jnp.float32),
            pltpu.VMEM((chunks * spans, LANES), jnp.float32),
            pltpu.SemaphoreType.DMA,
            pltpu.SemaphoreType.DMA((planes,)),
        ],
        compiler_params=pltpu.CompilerParams(collective_id=0, has_side_effects=True),
    )(owner_span_order, momentum, picked, *[jnp.asarray(c, dtype=jnp.bfloat16) for c in constants])


def local(groups, planes, momentum, picked, owner_span_order):
    entries = momentum.shape[0] * TOPK
    if entries % LANES == 0 and groups * planes * entries * 8 <= GATHER_BYTES:
        return local_small(groups, planes, momentum, picked, owner_span_order)
    return local_large(momentum, picked, owner_span_order)


def solution(mesh):
    return jax.shard_map(
        functools.partial(local, mesh.shape["grp"], mesh.shape["rep"]),
        mesh=mesh,
        in_specs=(P(("grp", "rep"), None), P(("grp", "rep"), None), P()),
        out_specs=(P(), P(("grp", "rep"), None)),
        check_vma=False,
    )
```

```python
import math

import functools

import jax
import jax.numpy as jnp
import numpy as np
from jax import lax
from jax.experimental import pallas as pl
from jax.experimental.pallas import tpu as pltpu
from jax.sharding import PartitionSpec as P

BLOCK = 64
TOPK = 32
CH_OWN = 1


def dct_cosines(points):
    freq = jnp.arange(points, dtype=jnp.float32)[:, None]
    place = jnp.arange(points, dtype=jnp.float32)[None, :]
    values = jnp.cos(jnp.pi * (2.0 * place + 1.0) * freq / (2.0 * points)) * jnp.sqrt(2.0 / points)
    values = values.at[0].multiply(jnp.sqrt(0.5))
    rounded = lax.optimization_barrier(values.astype(jnp.bfloat16))
    return rounded.astype(jnp.float32)


def forward(square_low, cosines, cos_low):
    half = jnp.einsum("cab,jb->caj", square_low, cos_low, preferred_element_type=jnp.float32)
    return jnp.einsum("ia,caj->cij", cosines, half, precision=lax.Precision.HIGHEST)


def decode(dense_matrix, cosines):
    square = dense_matrix.reshape(dense_matrix.shape[0], BLOCK, BLOCK)
    half = jnp.einsum("cij,jb->cib", square, cosines, precision=lax.Precision.HIGHEST)
    full = jnp.einsum("ia,cib->cab", cosines, half, precision=lax.Precision.HIGHEST)
    return full.reshape(dense_matrix.shape[0], BLOCK * BLOCK)


def decode_sparse(dense_low, cosines, cos_low):
    square = dense_low.reshape(dense_low.shape[0], BLOCK, BLOCK)
    half = jnp.einsum("cij,jb->cib", square, cos_low, preferred_element_type=jnp.float32)
    full = jnp.einsum("ia,cib->cab", cosines, half, precision=lax.Precision.HIGHEST)
    return full.reshape(dense_low.shape[0], BLOCK * BLOCK)


def densify(values, spots):
    entries, columns = values.shape
    per_step = math.gcd(entries, max(1, 65536 // columns))
    positions = jnp.arange(BLOCK, dtype=jnp.int32)

    def one_block(pieces):
        block_values, block_spots = pieces
        zeros = jnp.zeros_like(block_values)
        row_onehot = jnp.where(
            (block_spots // BLOCK)[:, None, :] == positions[None, :, None],
            block_values[:, None, :],
            zeros[:, None, :],
        )
        column_onehot = ((block_spots % BLOCK)[:, None, :] == positions[None, :, None]).astype(
            jnp.bfloat16
        )
        dense_matrix = jnp.einsum(
            "bcy,bzy->bcz", row_onehot, column_onehot, preferred_element_type=jnp.float32
        )
        return dense_matrix.reshape(per_step, BLOCK * BLOCK)

    stacked = lax.map(
        one_block,
        (
            values.reshape(entries // per_step, per_step, columns),
            spots.reshape(entries // per_step, per_step, columns),
        ),
    )
    return stacked.reshape(entries, BLOCK * BLOCK)


def owner_sum(received):
    values, spots = received
    return densify(values[0], spots[0])


def local_large(momentum, picked, owner_span_order):
    cosines = dct_cosines(BLOCK)
    cos_low = cosines.astype(jnp.bfloat16)
    owners = lax.axis_size("grp")
    span_count = momentum.shape[0]
    square_low = momentum.reshape(span_count, BLOCK, BLOCK)
    transform_coefficients = forward(square_low, cosines, cos_low).reshape(
        span_count, BLOCK * BLOCK
    )
    chosen = jnp.take_along_axis(transform_coefficients, picked, axis=1).astype(jnp.bfloat16)
    own_dense = densify(chosen, picked).astype(jnp.bfloat16)
    residual_momentum = (
        momentum.astype(jnp.float32) - decode_sparse(own_dense, cosines, cos_low)
    ).astype(jnp.bfloat16)
    slot_values = jnp.take(chosen, owner_span_order, axis=0)
    slot_spots = jnp.take(picked, owner_span_order, axis=0)
    shaped = (slot_values.reshape(owners, CH_OWN, TOPK), slot_spots.reshape(owners, CH_OWN, TOPK))
    partial_sum = owner_sum(
        (
            lax.all_to_all(shaped[0], "grp", split_axis=0, concat_axis=2, tiled=True),
            lax.all_to_all(shaped[1], "grp", split_axis=0, concat_axis=2, tiled=True),
        )
    )
    partial_sum = lax.psum(partial_sum, "rep")
    my_share = decode(partial_sum, cosines).astype(jnp.bfloat16)
    update = lax.all_gather(my_share, "grp", axis=0, tiled=True)
    return (update, residual_momentum)


LANES = 128
GATHER_BYTES = 2**20


def cosine_table():
    freq = np.arange(BLOCK, dtype=np.float64)[:, None]
    place = np.arange(BLOCK, dtype=np.float64)[None, :]
    values = np.cos(np.pi * (2 * place + 1) * freq / (2 * BLOCK)) * np.sqrt(2 / BLOCK)
    values[0] *= np.sqrt(0.5)
    return values.astype(np.float32)


def contract_lanes(left, right):
    return lax.dot_general(
        left, right, (((1,), (1,)), ((), ())), preferred_element_type=jnp.float32
    )


def matmul(left, right):
    return jnp.dot(left, right, preferred_element_type=jnp.float32)


def split(value):
    high = value.astype(jnp.bfloat16)
    return high, (value - high.astype(jnp.float32)).astype(jnp.bfloat16)


def exchange_kernel(
    groups,
    planes,
    order_ref,
    momentum_hbm,
    picked_hbm,
    rows_hbm,
    cols_hbm,
    twice_hbm,
    pairs_hbm,
    update_ref,
    residual_ref,
    momentum_ref,
    picked_ref,
    rows_ref,
    cols_ref,
    twice_ref,
    pairs_ref,
    value_box,
    spot_box,
    dense,
    decoded,
    load_sem,
    send_sem,
    value_sem,
    spot_sem,
):
    sources = (picked_hbm, cols_hbm, rows_hbm, momentum_hbm, twice_hbm, pairs_hbm)
    targets = (picked_ref, cols_ref, rows_ref, momentum_ref, twice_ref, pairs_ref)
    loads = [
        pltpu.make_async_copy(source, target, load_sem.at[n])
        for n, (source, target) in enumerate(zip(sources, targets))
    ]
    for load in loads:
        load.start()
    spans = momentum_ref.shape[0]
    entries = spans * TOPK
    chunks = BLOCK * BLOCK // LANES
    in_tile = LANES // TOPK
    tiles = entries // LANES
    devices = groups * planes
    my_group, my_plane = lax.axis_index("grp"), lax.axis_index("rep")
    group_of = [lax.rem(my_group + step, groups) for step in range(groups)]
    plane_of = [lax.rem(my_plane + step, planes) for step in range(planes)]

    def peer(plane, group):
        return {"grp": group_of[group], "rep": plane_of[plane]}

    others = [(z, g) for z in range(planes) for g in range(groups) if z or g]
    barrier = pltpu.get_barrier_semaphore()
    for z, g in others[::-1]:
        pl.semaphore_signal(barrier, inc=1, device_id=peer(z, g), device_id_type=pl.DeviceIdType.MESH)

    for load in loads:
        load.wait()
    lane = lax.broadcasted_iota(jnp.int32, (spans, entries), 1)
    mine = (lane // TOPK) == lax.broadcasted_iota(jnp.int32, (spans, entries), 0)
    spread = jnp.concatenate([picked_ref[...]] * spans, axis=1)
    spots = jnp.sum(jnp.where(mine, spread, 0), axis=0, keepdims=True)
    freq = lax.broadcasted_iota(jnp.int32, (BLOCK, entries), 0)
    one_row = jnp.where(freq == spots // BLOCK, 1.0, 0.0).astype(jnp.bfloat16)
    one_col = jnp.where(freq == spots % BLOCK, 1.0, 0.0).astype(jnp.bfloat16)
    half_rows = chunks * spans
    wave = matmul(cols_ref[...], one_col).astype(jnp.bfloat16)
    blank = jnp.zeros_like(wave)
    waves = (jnp.concatenate([wave, blank], axis=0), jnp.concatenate([blank, wave], axis=0))
    momentum = jnp.concatenate(
        [momentum_ref[:, k * LANES : (k + 1) * LANES].astype(jnp.float32) for k in range(chunks)],
        axis=0,
    )
    momentum_low = momentum.astype(jnp.bfloat16)
    total = jnp.zeros((spans, entries), jnp.float32)
    row_waves = []
    for p in range(2):
        row_wave = matmul(rows_ref[p * half_rows : (p + 1) * half_rows, :], one_row)
        row_waves.append(row_wave)
        product = row_wave * matmul(momentum_low, waves[p])
        total += jnp.sum(product.reshape(chunks, spans, entries), axis=0)
    chosen = jnp.sum(jnp.where(mine, total, 0.0), axis=0, keepdims=True)
    chosen_low = chosen.astype(jnp.bfloat16)
    chosen = chosen_low.astype(jnp.float32)

    def by_tile(row):
        return jnp.concatenate(
            [row[:, h * LANES : (h + 1) * LANES] for h in range(tiles)], axis=0
        )

    value_box[0] = by_tile(chosen).astype(jnp.bfloat16)
    spot_box[0] = by_tile(spots).astype(jnp.int16)

    pl.semaphore_wait(barrier, devices - 1)
    copies = []
    for z, g in others[::-1]:
        for box, arrived in ((spot_box, spot_sem), (value_box, value_sem)):
            copy = pltpu.make_async_remote_copy(
                src_ref=box.at[0],
                dst_ref=box.at[z * groups + g],
                send_sem=send_sem,
                recv_sem=arrived.at[z],
                device_id=peer(z, g),
                device_id_type=pl.DeviceIdType.MESH,
            )
            copy.start()
            copies.append(copy)

    correction = jnp.zeros((half_rows, LANES), jnp.float32)
    scaled = jnp.where(mine, chosen, 0.0)
    for p in range(2):
        weight = row_waves[p].reshape(chunks, spans, entries) * scaled[None]
        for part in split(weight.reshape(half_rows, entries)):
            correction += contract_lanes(part, waves[p])
    residual = momentum - correction
    for k in range(chunks):
        residual_ref[:, k * LANES : (k + 1) * LANES] = residual[
            k * spans : (k + 1) * spans
        ].astype(jnp.bfloat16)

    offset = (lax.broadcasted_iota(jnp.int32, (1, LANES), 1) // TOPK) * BLOCK
    tall = lax.broadcasted_iota(jnp.int32, (in_tile * BLOCK, LANES), 0)
    short = lax.broadcasted_iota(jnp.int32, (BLOCK, LANES), 0)
    sums = [jnp.zeros((in_tile * BLOCK, BLOCK), jnp.float32) for _ in range(tiles)]
    reach = sorted(range(planes), key=lambda z: min(z, planes - z))
    for z in reach:
        first = 1 if z == 0 else 0
        for box, arrived in ((spot_box, spot_sem), (value_box, value_sem)):
            landed = box.at[pl.ds(z * groups + first, groups - first)]
            pltpu.make_async_copy(landed, landed, arrived.at[z]).wait()
        values = [value_box[z * groups + g].astype(jnp.float32) for g in range(groups)]
        places = [spot_box[z * groups + g].astype(jnp.int32) for g in range(groups)]
        for h in range(tiles):
            left, right = [], []
            for g in range(groups):
                value = values[g][h : h + 1]
                spot = places[g][h : h + 1]
                left.append(jnp.where(tall == spot // BLOCK + offset, 1.0, 0.0).astype(jnp.bfloat16))
                right.append(jnp.where(short == spot % BLOCK, value, 0.0).astype(jnp.bfloat16))
            sums[h] += contract_lanes(
                jnp.concatenate(left, axis=1), jnp.concatenate(right, axis=1)
            )
    lower = lax.broadcasted_iota(jnp.int32, (BLOCK, LANES), 1) < BLOCK
    for h in range(tiles):
        half = sum(matmul(part, twice_ref[...]) for part in split(sums[h]))
        for c in range(in_tile):
            dense[h * in_tile + c] = half[c * BLOCK : (c + 1) * BLOCK]
    for s in range(spans):
        half = dense[order_ref[s]]
        stacked = jnp.concatenate(
            [jnp.where(lower, half, 0.0), jnp.where(lower, 0.0, half)], axis=0
        )
        decoded[pl.ds(s, chunks, stride=spans), :] = matmul(
            pairs_ref[...], stacked.astype(jnp.bfloat16)
        )
    for k in range(chunks):
        update_ref[:, k * LANES : (k + 1) * LANES] = decoded[
            k * spans : (k + 1) * spans, :
        ].astype(jnp.bfloat16)
    for copy in copies:
        copy.wait_send()


def store_kernel(update_ref, residual_ref, update_hbm, residual_hbm, sem):
    stores = [
        pltpu.make_async_copy(residual_ref, residual_hbm, sem.at[0]),
        pltpu.make_async_copy(update_ref, update_hbm, sem.at[1]),
    ]
    for store in stores:
        store.start()
    for store in stores:
        store.wait()


def local_small(groups, planes, momentum, picked, owner_span_order):
    spans = momentum.shape[0]
    chunks = BLOCK * BLOCK // LANES
    table = cosine_table()
    by_pair = table.T.reshape(chunks, 2, BLOCK)
    rows = np.repeat(by_pair.transpose(1, 0, 2), spans, axis=1).reshape(-1, BLOCK)
    constants = [rows, table.T, np.concatenate([table, table], axis=1), by_pair.reshape(chunks, LANES)]
    constants = [jnp.asarray(constant, dtype=jnp.bfloat16) for constant in constants]
    operands = [momentum, picked, *constants]
    anywhere = pl.BlockSpec(memory_space=pl.ANY)
    vmem = pl.BlockSpec(memory_space=pltpu.VMEM)
    devices = groups * planes
    box_shape = (devices, spans * TOPK // LANES, LANES)
    results = pl.pallas_call(
        functools.partial(exchange_kernel, groups, planes),
        out_shape=[pltpu.VMEM(momentum.shape, jnp.bfloat16)] * 2,
        in_specs=[pl.BlockSpec(memory_space=pltpu.SMEM)] + [anywhere] * len(operands),
        out_specs=[vmem] * 2,
        scratch_shapes=[pltpu.VMEM(x.shape, x.dtype) for x in operands]
        + [
            pltpu.VMEM(box_shape, jnp.bfloat16),
            pltpu.VMEM(box_shape, jnp.int16),
            pltpu.VMEM((spans, BLOCK, LANES), jnp.float32),
            pltpu.VMEM((chunks * spans, LANES), jnp.float32),
            pltpu.SemaphoreType.DMA((len(operands),)),
            pltpu.SemaphoreType.DMA,
            pltpu.SemaphoreType.DMA((planes,)),
            pltpu.SemaphoreType.DMA((planes,)),
        ],
        compiler_params=pltpu.CompilerParams(collective_id=0, has_side_effects=True),
    )(owner_span_order, *operands)
    return pl.pallas_call(
        store_kernel,
        out_shape=[jax.ShapeDtypeStruct(momentum.shape, jnp.bfloat16)] * 2,
        in_specs=[vmem] * 2,
        out_specs=[anywhere] * 2,
        scratch_shapes=[pltpu.SemaphoreType.DMA((2,))],
    )(*[pltpu.with_memory_space_constraint(result, pltpu.VMEM) for result in results])


def local(groups, planes, momentum, picked, owner_span_order):
    entries = momentum.shape[0] * TOPK
    if entries % LANES == 0 and groups * planes * entries * 8 <= GATHER_BYTES:
        return local_small(groups, planes, momentum, picked, owner_span_order)
    return local_large(momentum, picked, owner_span_order)


def solution(mesh):
    return jax.shard_map(
        functools.partial(local, mesh.shape["grp"], mesh.shape["rep"]),
        mesh=mesh,
        in_specs=(P(("grp", "rep"), None), P(("grp", "rep"), None), P()),
        out_specs=(P(), P(("grp", "rep"), None)),
        check_vma=False,
    )
```

```python
import math

import functools

import jax
import jax.numpy as jnp
import numpy as np
from jax import lax
from jax.experimental import pallas as pl
from jax.experimental.pallas import tpu as pltpu
from jax.sharding import PartitionSpec as P

BLOCK = 64
TOPK = 32
CH_OWN = 1


def dct_cosines(points):
    freq = jnp.arange(points, dtype=jnp.float32)[:, None]
    place = jnp.arange(points, dtype=jnp.float32)[None, :]
    values = jnp.cos(jnp.pi * (2.0 * place + 1.0) * freq / (2.0 * points)) * jnp.sqrt(2.0 / points)
    values = values.at[0].multiply(jnp.sqrt(0.5))
    rounded = lax.optimization_barrier(values.astype(jnp.bfloat16))
    return rounded.astype(jnp.float32)


def forward(square_low, cosines, cos_low):
    half = jnp.einsum("cab,jb->caj", square_low, cos_low, preferred_element_type=jnp.float32)
    return jnp.einsum("ia,caj->cij", cosines, half, precision=lax.Precision.HIGHEST)


def decode(dense_matrix, cosines):
    square = dense_matrix.reshape(dense_matrix.shape[0], BLOCK, BLOCK)
    half = jnp.einsum("cij,jb->cib", square, cosines, precision=lax.Precision.HIGHEST)
    full = jnp.einsum("ia,cib->cab", cosines, half, precision=lax.Precision.HIGHEST)
    return full.reshape(dense_matrix.shape[0], BLOCK * BLOCK)


def decode_sparse(dense_low, cosines, cos_low):
    square = dense_low.reshape(dense_low.shape[0], BLOCK, BLOCK)
    half = jnp.einsum("cij,jb->cib", square, cos_low, preferred_element_type=jnp.float32)
    full = jnp.einsum("ia,cib->cab", cosines, half, precision=lax.Precision.HIGHEST)
    return full.reshape(dense_low.shape[0], BLOCK * BLOCK)


def densify(values, spots):
    entries, columns = values.shape
    per_step = math.gcd(entries, max(1, 65536 // columns))
    positions = jnp.arange(BLOCK, dtype=jnp.int32)

    def one_block(pieces):
        block_values, block_spots = pieces
        zeros = jnp.zeros_like(block_values)
        row_onehot = jnp.where(
            (block_spots // BLOCK)[:, None, :] == positions[None, :, None],
            block_values[:, None, :],
            zeros[:, None, :],
        )
        column_onehot = ((block_spots % BLOCK)[:, None, :] == positions[None, :, None]).astype(
            jnp.bfloat16
        )
        dense_matrix = jnp.einsum(
            "bcy,bzy->bcz", row_onehot, column_onehot, preferred_element_type=jnp.float32
        )
        return dense_matrix.reshape(per_step, BLOCK * BLOCK)

    stacked = lax.map(
        one_block,
        (
            values.reshape(entries // per_step, per_step, columns),
            spots.reshape(entries // per_step, per_step, columns),
        ),
    )
    return stacked.reshape(entries, BLOCK * BLOCK)


def owner_sum(received):
    values, spots = received
    return densify(values[0], spots[0])


def local_large(momentum, picked, owner_span_order):
    cosines = dct_cosines(BLOCK)
    cos_low = cosines.astype(jnp.bfloat16)
    owners = lax.axis_size("grp")
    span_count = momentum.shape[0]
    square_low = momentum.reshape(span_count, BLOCK, BLOCK)
    transform_coefficients = forward(square_low, cosines, cos_low).reshape(
        span_count, BLOCK * BLOCK
    )
    chosen = jnp.take_along_axis(transform_coefficients, picked, axis=1).astype(jnp.bfloat16)
    own_dense = densify(chosen, picked).astype(jnp.bfloat16)
    residual_momentum = (
        momentum.astype(jnp.float32) - decode_sparse(own_dense, cosines, cos_low)
    ).astype(jnp.bfloat16)
    slot_values = jnp.take(chosen, owner_span_order, axis=0)
    slot_spots = jnp.take(picked, owner_span_order, axis=0)
    shaped = (slot_values.reshape(owners, CH_OWN, TOPK), slot_spots.reshape(owners, CH_OWN, TOPK))
    partial_sum = owner_sum(
        (
            lax.all_to_all(shaped[0], "grp", split_axis=0, concat_axis=2, tiled=True),
            lax.all_to_all(shaped[1], "grp", split_axis=0, concat_axis=2, tiled=True),
        )
    )
    partial_sum = lax.psum(partial_sum, "rep")
    my_share = decode(partial_sum, cosines).astype(jnp.bfloat16)
    update = lax.all_gather(my_share, "grp", axis=0, tiled=True)
    return (update, residual_momentum)


LANES = 128
GATHER_BYTES = 2**20


def cosine_table():
    freq = np.arange(BLOCK, dtype=np.float64)[:, None]
    place = np.arange(BLOCK, dtype=np.float64)[None, :]
    values = np.cos(np.pi * (2 * place + 1) * freq / (2 * BLOCK)) * np.sqrt(2 / BLOCK)
    values[0] *= np.sqrt(0.5)
    return values.astype(np.float32)


def contract_lanes(left, right):
    return lax.dot_general(
        left, right, (((1,), (1,)), ((), ())), preferred_element_type=jnp.float32
    )


def matmul(left, right):
    return jnp.dot(left, right, preferred_element_type=jnp.float32)


def split(value):
    high = value.astype(jnp.bfloat16)
    return high, (value - high.astype(jnp.float32)).astype(jnp.bfloat16)


def exchange_kernel(
    groups,
    planes,
    order_hbm,
    momentum_hbm,
    picked_hbm,
    rows_hbm,
    cols_hbm,
    twice_hbm,
    pairs_hbm,
    update_ref,
    residual_ref,
    order_ref,
    momentum_ref,
    picked_ref,
    rows_ref,
    cols_ref,
    twice_ref,
    pairs_ref,
    value_box,
    spot_box,
    dense,
    decoded,
    load_sem,
    send_sem,
    value_sem,
    spot_sem,
):
    sources = (picked_hbm, cols_hbm, rows_hbm, momentum_hbm, twice_hbm, pairs_hbm, order_hbm)
    targets = (picked_ref, cols_ref, rows_ref, momentum_ref, twice_ref, pairs_ref, order_ref)
    loads = [
        pltpu.make_async_copy(source, target, load_sem.at[n])
        for n, (source, target) in enumerate(zip(sources, targets))
    ]
    spans = momentum_ref.shape[0]
    entries = spans * TOPK
    chunks = BLOCK * BLOCK // LANES
    in_tile = LANES // TOPK
    tiles = entries // LANES
    devices = groups * planes
    my_group, my_plane = lax.axis_index("grp"), lax.axis_index("rep")
    group_of = [lax.rem(my_group + step, groups) for step in range(groups)]
    plane_of = [lax.rem(my_plane + step, planes) for step in range(planes)]

    def peer(plane, group):
        return {"grp": group_of[group], "rep": plane_of[plane]}

    others = [(z, g) for z in range(planes) for g in range(groups) if z or g]
    barrier = pltpu.get_barrier_semaphore()
    for z, g in others[::-1]:
        pl.semaphore_signal(barrier, inc=1, device_id=peer(z, g), device_id_type=pl.DeviceIdType.MESH)

    for load in loads:
        load.start()
    for load in loads:
        load.wait()
    lane = lax.broadcasted_iota(jnp.int32, (spans, entries), 1)
    mine = (lane // TOPK) == lax.broadcasted_iota(jnp.int32, (spans, entries), 0)
    spread = jnp.concatenate([picked_ref[...]] * spans, axis=1)
    spots = jnp.sum(jnp.where(mine, spread, 0), axis=0, keepdims=True)
    freq = lax.broadcasted_iota(jnp.int32, (BLOCK, entries), 0)
    one_row = jnp.where(freq == spots // BLOCK, 1.0, 0.0).astype(jnp.bfloat16)
    one_col = jnp.where(freq == spots % BLOCK, 1.0, 0.0).astype(jnp.bfloat16)
    half_rows = chunks * spans
    wave = matmul(cols_ref[...], one_col).astype(jnp.bfloat16)
    blank = jnp.zeros_like(wave)
    waves = (jnp.concatenate([wave, blank], axis=0), jnp.concatenate([blank, wave], axis=0))
    momentum = jnp.concatenate(
        [momentum_ref[:, k * LANES : (k + 1) * LANES].astype(jnp.float32) for k in range(chunks)],
        axis=0,
    )
    momentum_low = momentum.astype(jnp.bfloat16)
    total = jnp.zeros((spans, entries), jnp.float32)
    row_waves = []
    for p in range(2):
        row_wave = matmul(rows_ref[p * half_rows : (p + 1) * half_rows, :], one_row)
        row_waves.append(row_wave)
        product = row_wave * matmul(momentum_low, waves[p])
        total += jnp.sum(product.reshape(chunks, spans, entries), axis=0)
    chosen = jnp.sum(jnp.where(mine, total, 0.0), axis=0, keepdims=True)
    chosen_low = chosen.astype(jnp.bfloat16)
    chosen = chosen_low.astype(jnp.float32)

    def by_tile(row):
        return jnp.concatenate(
            [row[:, h * LANES : (h + 1) * LANES] for h in range(tiles)], axis=0
        )

    value_box[0] = by_tile(chosen).astype(jnp.bfloat16)
    spot_box[0] = by_tile(spots).astype(jnp.int16)

    pl.semaphore_wait(barrier, devices - 1)
    copies = []
    for z, g in others[::-1]:
        for box, arrived in ((spot_box, spot_sem), (value_box, value_sem)):
            copy = pltpu.make_async_remote_copy(
                src_ref=box.at[0],
                dst_ref=box.at[z * groups + g],
                send_sem=send_sem,
                recv_sem=arrived.at[z],
                device_id=peer(z, g),
                device_id_type=pl.DeviceIdType.MESH,
            )
            copy.start()
            copies.append(copy)

    correction = jnp.zeros((half_rows, LANES), jnp.float32)
    scaled = jnp.where(mine, chosen, 0.0)
    for p in range(2):
        weight = row_waves[p].reshape(chunks, spans, entries) * scaled[None]
        for part in split(weight.reshape(half_rows, entries)):
            correction += contract_lanes(part, waves[p])
    residual = momentum - correction
    for k in range(chunks):
        residual_ref[:, k * LANES : (k + 1) * LANES] = residual[
            k * spans : (k + 1) * spans
        ].astype(jnp.bfloat16)

    offset = (lax.broadcasted_iota(jnp.int32, (1, LANES), 1) // TOPK) * BLOCK
    tall = lax.broadcasted_iota(jnp.int32, (in_tile * BLOCK, LANES), 0)
    tall = tall.astype(jnp.float32).astype(jnp.bfloat16)
    short = tall[:BLOCK]
    one, zero = jnp.ones((), jnp.bfloat16), jnp.zeros((), jnp.bfloat16)

    def low(integers):
        return integers.astype(jnp.float32).astype(jnp.bfloat16)

    sums = [jnp.zeros((in_tile * BLOCK, BLOCK), jnp.float32) for _ in range(tiles)]
    reach = sorted(range(planes), key=lambda z: min(z, planes - z))
    for z in reach:
        first = 1 if z == 0 else 0
        for box, arrived in ((spot_box, spot_sem), (value_box, value_sem)):
            landed = box.at[pl.ds(z * groups + first, groups - first)]
            pltpu.make_async_copy(landed, landed, arrived.at[z]).wait()
        values = [value_box[z * groups + g] for g in range(groups)]
        places = [spot_box[z * groups + g].astype(jnp.int32) for g in range(groups)]
        for h in range(tiles):
            left, right = [], []
            for g in range(groups):
                value = values[g][h : h + 1]
                spot = places[g][h : h + 1]
                left.append(jnp.where(tall == low(spot // BLOCK + offset), one, zero))
                right.append(jnp.where(short == low(spot % BLOCK), value, zero))
            sums[h] += contract_lanes(
                jnp.concatenate(left, axis=1), jnp.concatenate(right, axis=1)
            )
    lower = lax.broadcasted_iota(jnp.int32, (BLOCK, LANES), 1) < BLOCK
    for h in range(tiles):
        half = sum(matmul(part, twice_ref[...]) for part in split(sums[h]))
        for c in range(in_tile):
            dense[h * in_tile + c] = half[c * BLOCK : (c + 1) * BLOCK]
    for s in range(spans):
        half = dense[order_ref[s]]
        stacked = jnp.concatenate(
            [jnp.where(lower, half, 0.0), jnp.where(lower, 0.0, half)], axis=0
        )
        decoded[pl.ds(s, chunks, stride=spans), :] = matmul(
            pairs_ref[...], stacked.astype(jnp.bfloat16)
        )
    for k in range(chunks):
        update_ref[:, k * LANES : (k + 1) * LANES] = decoded[
            k * spans : (k + 1) * spans, :
        ].astype(jnp.bfloat16)
    for copy in copies:
        copy.wait_send()


def store_kernel(update_ref, residual_ref, update_hbm, residual_hbm, sem):
    stores = [
        pltpu.make_async_copy(residual_ref, residual_hbm, sem.at[0]),
        pltpu.make_async_copy(update_ref, update_hbm, sem.at[1]),
    ]
    for store in stores:
        store.start()
    for store in stores:
        store.wait()


def local_small(groups, planes, momentum, picked, owner_span_order):
    spans = momentum.shape[0]
    chunks = BLOCK * BLOCK // LANES
    table = cosine_table()
    by_pair = table.T.reshape(chunks, 2, BLOCK)
    rows = np.repeat(by_pair.transpose(1, 0, 2), spans, axis=1).reshape(-1, BLOCK)
    constants = [rows, table.T, np.concatenate([table, table], axis=1), by_pair.reshape(chunks, LANES)]
    constants = [jnp.asarray(constant, dtype=jnp.bfloat16) for constant in constants]
    operands = [owner_span_order, momentum, picked, *constants]
    anywhere = pl.BlockSpec(memory_space=pl.ANY)
    vmem = pl.BlockSpec(memory_space=pltpu.VMEM)
    devices = groups * planes
    box_shape = (devices, spans * TOPK // LANES, LANES)
    results = pl.pallas_call(
        functools.partial(exchange_kernel, groups, planes),
        out_shape=[pltpu.VMEM(momentum.shape, jnp.bfloat16)] * 2,
        in_specs=[anywhere] * len(operands),
        out_specs=[vmem] * 2,
        scratch_shapes=[pltpu.SMEM(owner_span_order.shape, jnp.int32)]
        + [pltpu.VMEM(x.shape, x.dtype) for x in operands[1:]]
        + [
            pltpu.VMEM(box_shape, jnp.bfloat16),
            pltpu.VMEM(box_shape, jnp.int16),
            pltpu.VMEM((spans, BLOCK, LANES), jnp.float32),
            pltpu.VMEM((chunks * spans, LANES), jnp.float32),
            pltpu.SemaphoreType.DMA((len(operands),)),
            pltpu.SemaphoreType.DMA,
            pltpu.SemaphoreType.DMA((planes,)),
            pltpu.SemaphoreType.DMA((planes,)),
        ],
        compiler_params=pltpu.CompilerParams(collective_id=0, has_side_effects=True),
    )(*operands)
    return pl.pallas_call(
        store_kernel,
        out_shape=[jax.ShapeDtypeStruct(momentum.shape, jnp.bfloat16)] * 2,
        in_specs=[vmem] * 2,
        out_specs=[anywhere] * 2,
        scratch_shapes=[pltpu.SemaphoreType.DMA((2,))],
    )(*[pltpu.with_memory_space_constraint(result, pltpu.VMEM) for result in results])


def local(groups, planes, momentum, picked, owner_span_order):
    entries = momentum.shape[0] * TOPK
    if entries % LANES == 0 and groups * planes * entries * 8 <= GATHER_BYTES:
        return local_small(groups, planes, momentum, picked, owner_span_order)
    return local_large(momentum, picked, owner_span_order)


def solution(mesh):
    return jax.shard_map(
        functools.partial(local, mesh.shape["grp"], mesh.shape["rep"]),
        mesh=mesh,
        in_specs=(P(("grp", "rep"), None), P(("grp", "rep"), None), P()),
        out_specs=(P(), P(("grp", "rep"), None)),
        check_vma=False,
    )
```

```python
import math

import functools

import jax
import jax.numpy as jnp
import numpy as np
from jax import lax
from jax.experimental import pallas as pl
from jax.experimental.pallas import tpu as pltpu
from jax.sharding import PartitionSpec as P

BLOCK = 64
TOPK = 32
CH_OWN = 1


def dct_cosines(points):
    freq = jnp.arange(points, dtype=jnp.float32)[:, None]
    place = jnp.arange(points, dtype=jnp.float32)[None, :]
    values = jnp.cos(jnp.pi * (2.0 * place + 1.0) * freq / (2.0 * points)) * jnp.sqrt(2.0 / points)
    values = values.at[0].multiply(jnp.sqrt(0.5))
    rounded = lax.optimization_barrier(values.astype(jnp.bfloat16))
    return rounded.astype(jnp.float32)


def forward(square_low, cosines, cos_low):
    half = jnp.einsum("cab,jb->caj", square_low, cos_low, preferred_element_type=jnp.float32)
    return jnp.einsum("ia,caj->cij", cosines, half, precision=lax.Precision.HIGHEST)


def decode(dense_matrix, cosines):
    square = dense_matrix.reshape(dense_matrix.shape[0], BLOCK, BLOCK)
    half = jnp.einsum("cij,jb->cib", square, cosines, precision=lax.Precision.HIGHEST)
    full = jnp.einsum("ia,cib->cab", cosines, half, precision=lax.Precision.HIGHEST)
    return full.reshape(dense_matrix.shape[0], BLOCK * BLOCK)


def decode_sparse(dense_low, cosines, cos_low):
    square = dense_low.reshape(dense_low.shape[0], BLOCK, BLOCK)
    half = jnp.einsum("cij,jb->cib", square, cos_low, preferred_element_type=jnp.float32)
    full = jnp.einsum("ia,cib->cab", cosines, half, precision=lax.Precision.HIGHEST)
    return full.reshape(dense_low.shape[0], BLOCK * BLOCK)


def densify(values, spots):
    entries, columns = values.shape
    per_step = math.gcd(entries, max(1, 65536 // columns))
    positions = jnp.arange(BLOCK, dtype=jnp.int32)

    def one_block(pieces):
        block_values, block_spots = pieces
        zeros = jnp.zeros_like(block_values)
        row_onehot = jnp.where(
            (block_spots // BLOCK)[:, None, :] == positions[None, :, None],
            block_values[:, None, :],
            zeros[:, None, :],
        )
        column_onehot = ((block_spots % BLOCK)[:, None, :] == positions[None, :, None]).astype(
            jnp.bfloat16
        )
        dense_matrix = jnp.einsum(
            "bcy,bzy->bcz", row_onehot, column_onehot, preferred_element_type=jnp.float32
        )
        return dense_matrix.reshape(per_step, BLOCK * BLOCK)

    stacked = lax.map(
        one_block,
        (
            values.reshape(entries // per_step, per_step, columns),
            spots.reshape(entries // per_step, per_step, columns),
        ),
    )
    return stacked.reshape(entries, BLOCK * BLOCK)


def owner_sum(received):
    values, spots = received
    return densify(values[0], spots[0])


def local_large(momentum, picked, owner_span_order):
    cosines = dct_cosines(BLOCK)
    cos_low = cosines.astype(jnp.bfloat16)
    owners = lax.axis_size("grp")
    span_count = momentum.shape[0]
    square_low = momentum.reshape(span_count, BLOCK, BLOCK)
    transform_coefficients = forward(square_low, cosines, cos_low).reshape(
        span_count, BLOCK * BLOCK
    )
    chosen = jnp.take_along_axis(transform_coefficients, picked, axis=1).astype(jnp.bfloat16)
    own_dense = densify(chosen, picked).astype(jnp.bfloat16)
    residual_momentum = (
        momentum.astype(jnp.float32) - decode_sparse(own_dense, cosines, cos_low)
    ).astype(jnp.bfloat16)
    slot_values = jnp.take(chosen, owner_span_order, axis=0)
    slot_spots = jnp.take(picked, owner_span_order, axis=0)
    shaped = (slot_values.reshape(owners, CH_OWN, TOPK), slot_spots.reshape(owners, CH_OWN, TOPK))
    partial_sum = owner_sum(
        (
            lax.all_to_all(shaped[0], "grp", split_axis=0, concat_axis=2, tiled=True),
            lax.all_to_all(shaped[1], "grp", split_axis=0, concat_axis=2, tiled=True),
        )
    )
    partial_sum = lax.psum(partial_sum, "rep")
    my_share = decode(partial_sum, cosines).astype(jnp.bfloat16)
    update = lax.all_gather(my_share, "grp", axis=0, tiled=True)
    return (update, residual_momentum)


LANES = 128
GATHER_BYTES = 2**20


def cosine_table():
    freq = np.arange(BLOCK, dtype=np.float64)[:, None]
    place = np.arange(BLOCK, dtype=np.float64)[None, :]
    values = np.cos(np.pi * (2 * place + 1) * freq / (2 * BLOCK)) * np.sqrt(2 / BLOCK)
    values[0] *= np.sqrt(0.5)
    return values.astype(np.float32)


def contract_lanes(left, right):
    return lax.dot_general(
        left, right, (((1,), (1,)), ((), ())), preferred_element_type=jnp.float32
    )


def matmul(left, right):
    return jnp.dot(left, right, preferred_element_type=jnp.float32)


def split(value):
    high = value.astype(jnp.bfloat16)
    return high, (value - high.astype(jnp.float32)).astype(jnp.bfloat16)


def exchange_kernel(
    groups,
    planes,
    order_hbm,
    momentum_hbm,
    picked_hbm,
    rows_hbm,
    cols_hbm,
    twice_hbm,
    pairs_hbm,
    update_ref,
    residual_ref,
    order_ref,
    momentum_ref,
    picked_ref,
    rows_ref,
    cols_ref,
    twice_ref,
    pairs_ref,
    value_box,
    spot_box,
    turned_value,
    turned_spot,
    dense,
    decoded,
    load_sem,
    send_sem,
    value_sem,
    spot_sem,
):
    sources = (picked_hbm, cols_hbm, rows_hbm, momentum_hbm, twice_hbm, pairs_hbm, order_hbm)
    targets = (picked_ref, cols_ref, rows_ref, momentum_ref, twice_ref, pairs_ref, order_ref)
    loads = [
        pltpu.make_async_copy(source, target, load_sem.at[n])
        for n, (source, target) in enumerate(zip(sources, targets))
    ]
    for load in loads:
        load.start()
    spans = momentum_ref.shape[0]
    entries = spans * TOPK
    chunks = BLOCK * BLOCK // LANES
    in_tile = LANES // TOPK
    tiles = entries // LANES
    devices = groups * planes
    my_group, my_plane = lax.axis_index("grp"), lax.axis_index("rep")
    group_of = [lax.rem(my_group + step, groups) for step in range(groups)]
    plane_of = [lax.rem(my_plane + step, planes) for step in range(planes)]

    def peer(plane, group):
        return {"grp": group_of[group], "rep": plane_of[plane]}

    others = [(z, g) for z in range(planes) for g in range(groups) if z or g]
    far_first = [o for o in others if o[0]] + [o for o in others if not o[0]]
    barrier = pltpu.get_barrier_semaphore()
    for z, g in far_first:
        pl.semaphore_signal(barrier, inc=1, device_id=peer(z, g), device_id_type=pl.DeviceIdType.MESH)

    loads[0].wait()
    lane = lax.broadcasted_iota(jnp.int32, (spans, entries), 1)
    mine = (lane // TOPK) == lax.broadcasted_iota(jnp.int32, (spans, entries), 0)
    spread = jnp.concatenate([picked_ref[...]] * spans, axis=1)
    spots = jnp.sum(jnp.where(mine, spread, 0), axis=0, keepdims=True)
    freq = lax.broadcasted_iota(jnp.int32, (BLOCK, entries), 0)
    one_row = jnp.where(freq == spots // BLOCK, 1.0, 0.0).astype(jnp.bfloat16)
    one_col = jnp.where(freq == spots % BLOCK, 1.0, 0.0).astype(jnp.bfloat16)
    half_rows = chunks * spans
    for load in loads[1:]:
        load.wait()
    wave = matmul(cols_ref[...], one_col).astype(jnp.bfloat16)
    blank = jnp.zeros_like(wave)
    waves = (jnp.concatenate([wave, blank], axis=0), jnp.concatenate([blank, wave], axis=0))
    momentum = jnp.concatenate(
        [momentum_ref[:, k * LANES : (k + 1) * LANES].astype(jnp.float32) for k in range(chunks)],
        axis=0,
    )
    momentum_low = momentum.astype(jnp.bfloat16)
    total = jnp.zeros((spans, entries), jnp.float32)
    row_waves = []
    for p in range(2):
        row_wave = matmul(rows_ref[p * half_rows : (p + 1) * half_rows, :], one_row)
        row_waves.append(row_wave)
        product = row_wave * matmul(momentum_low, waves[p])
        total += jnp.sum(product.reshape(chunks, spans, entries), axis=0)
    chosen = jnp.sum(jnp.where(mine, total, 0.0), axis=0, keepdims=True)
    chosen_low = chosen.astype(jnp.bfloat16)
    chosen = chosen_low.astype(jnp.float32)

    def by_tile(row):
        return jnp.concatenate(
            [row[:, h * LANES : (h + 1) * LANES] for h in range(tiles)], axis=0
        )

    value_tile, spot_tile = by_tile(chosen), by_tile(spots)
    value_box[0] = value_tile.astype(jnp.bfloat16)
    spot_box[0] = spot_tile.astype(jnp.int16)
    for turn in range(in_tile):
        turned_value[turn] = pltpu.roll(value_tile, turn * TOPK, 1).astype(jnp.bfloat16)
        turned_spot[turn] = pltpu.roll(spot_tile, turn * TOPK, 1).astype(jnp.int16)

    pl.semaphore_wait(barrier, devices - 1)
    copies = []
    for z, g in far_first:
        for box, turned, arrived in (
            (spot_box, turned_spot, spot_sem),
            (value_box, turned_value, value_sem),
        ):
            copy = pltpu.make_async_remote_copy(
                src_ref=turned.at[g % in_tile],
                dst_ref=box.at[z * groups + g],
                send_sem=send_sem,
                recv_sem=arrived.at[z],
                device_id=peer(z, g),
                device_id_type=pl.DeviceIdType.MESH,
            )
            copy.start()
            copies.append(copy)

    def store_residual():
        correction = jnp.zeros((half_rows, LANES), jnp.float32)
        scaled = jnp.where(mine, chosen, 0.0)
        for p in range(2):
            weight = row_waves[p].reshape(chunks, spans, entries) * scaled[None]
            for part in split(weight.reshape(half_rows, entries)):
                correction += contract_lanes(part, waves[p])
        residual = momentum - correction
        for k in range(chunks):
            residual_ref[:, k * LANES : (k + 1) * LANES] = residual[
                k * spans : (k + 1) * spans
            ].astype(jnp.bfloat16)

    store_residual()
    block = lax.broadcasted_iota(jnp.int32, (tiles, LANES), 1) // TOPK
    taken = [block == turn for turn in range(in_tile)]
    freq = lax.broadcasted_iota(jnp.int32, (BLOCK, groups * TOPK), 0)
    freq = freq.astype(jnp.float32).astype(jnp.bfloat16)
    one, zero = jnp.ones((), jnp.bfloat16), jnp.zeros((), jnp.bfloat16)

    def low(integers):
        return integers.astype(jnp.float32).astype(jnp.bfloat16)

    def span_rows(rows, c):
        picks = []
        for first in range(0, groups, in_tile):
            row = rows[first]
            for turn in range(1, in_tile):
                row = jnp.where(taken[(c + turn) % in_tile], rows[first + turn], row)
            picks.append(row)
        return jnp.concatenate(picks, axis=1)

    sums = [None] * spans
    for z in range(planes):
        first = 1 if z == 0 else 0
        for box, arrived in ((spot_box, spot_sem), (value_box, value_sem)):
            landed = box.at[pl.ds(z * groups + first, groups - first)]
            pltpu.make_async_copy(landed, landed, arrived.at[z]).wait()
        values = [value_box[z * groups + g].astype(jnp.float32) for g in range(groups)]
        places = [spot_box[z * groups + g].astype(jnp.int32) for g in range(groups)]
        for c in range(in_tile):
            value = span_rows(values, c).astype(jnp.bfloat16)
            place = span_rows(places, c)
            row, column = low(place // BLOCK), low(place % BLOCK)
            for h in range(tiles):
                left = jnp.where(freq == row[h : h + 1], one, zero)
                right = jnp.where(freq == column[h : h + 1], value[h : h + 1], zero)
                part = contract_lanes(left, right)
                span = h * in_tile + c
                sums[span] = part if z == 0 else sums[span] + part
    for span in range(spans):
        dense[span] = matmul(sums[span].astype(jnp.bfloat16), twice_ref[...])
    lower = lax.broadcasted_iota(jnp.int32, (chunks, LANES), 1) < BLOCK
    for s in range(spans):
        full = matmul(pairs_ref[...], dense[order_ref[s]].astype(jnp.bfloat16))
        decoded[pl.ds(s, chunks, stride=spans), :] = jnp.where(
            lower, full[:chunks], full[chunks:]
        )
    for k in range(chunks):
        update_ref[:, k * LANES : (k + 1) * LANES] = decoded[
            k * spans : (k + 1) * spans, :
        ].astype(jnp.bfloat16)
    for copy in copies:
        copy.wait_send()


def store_kernel(update_ref, residual_ref, update_hbm, residual_hbm, sem):
    stores = [
        pltpu.make_async_copy(residual_ref, residual_hbm, sem.at[0]),
        pltpu.make_async_copy(update_ref, update_hbm, sem.at[1]),
    ]
    for store in stores:
        store.start()
    for store in stores:
        store.wait()


def local_small(groups, planes, momentum, picked, owner_span_order):
    spans = momentum.shape[0]
    chunks = BLOCK * BLOCK // LANES
    table = cosine_table()
    by_pair = table.T.reshape(chunks, 2, BLOCK)
    rows = np.repeat(by_pair.transpose(1, 0, 2), spans, axis=1).reshape(-1, BLOCK)
    constants = [rows, table.T, np.concatenate([table, table], axis=1), by_pair.transpose(1, 0, 2).reshape(-1, BLOCK)]
    constants = [jnp.asarray(constant, dtype=jnp.bfloat16) for constant in constants]
    operands = [owner_span_order, momentum, picked, *constants]
    anywhere = pl.BlockSpec(memory_space=pl.ANY)
    vmem = pl.BlockSpec(memory_space=pltpu.VMEM)
    devices = groups * planes
    turned_shape = (LANES // TOPK, spans * TOPK // LANES, LANES)
    box_shape = (devices, spans * TOPK // LANES, LANES)
    results = pl.pallas_call(
        functools.partial(exchange_kernel, groups, planes),
        out_shape=[pltpu.VMEM(momentum.shape, jnp.bfloat16)] * 2,
        in_specs=[anywhere] * len(operands),
        out_specs=[vmem] * 2,
        scratch_shapes=[pltpu.SMEM(owner_span_order.shape, jnp.int32)]
        + [pltpu.VMEM(x.shape, x.dtype) for x in operands[1:]]
        + [
            pltpu.VMEM(box_shape, jnp.bfloat16),
            pltpu.VMEM(box_shape, jnp.int16),
            pltpu.VMEM(turned_shape, jnp.bfloat16),
            pltpu.VMEM(turned_shape, jnp.int16),
            pltpu.VMEM((spans, BLOCK, LANES), jnp.float32),
            pltpu.VMEM((chunks * spans, LANES), jnp.float32),
            pltpu.SemaphoreType.DMA((len(operands),)),
            pltpu.SemaphoreType.DMA,
            pltpu.SemaphoreType.DMA((planes,)),
            pltpu.SemaphoreType.DMA((planes,)),
        ],
        compiler_params=pltpu.CompilerParams(collective_id=0, has_side_effects=True),
    )(*operands)
    return pl.pallas_call(
        store_kernel,
        out_shape=[jax.ShapeDtypeStruct(momentum.shape, jnp.bfloat16)] * 2,
        in_specs=[vmem] * 2,
        out_specs=[anywhere] * 2,
        scratch_shapes=[pltpu.SemaphoreType.DMA((2,))],
    )(*[pltpu.with_memory_space_constraint(result, pltpu.VMEM) for result in results])


def local(groups, planes, momentum, picked, owner_span_order):
    entries = momentum.shape[0] * TOPK
    if entries % LANES == 0 and groups % (LANES // TOPK) == 0 and groups * planes * entries * 8 <= GATHER_BYTES:
        return local_small(groups, planes, momentum, picked, owner_span_order)
    return local_large(momentum, picked, owner_span_order)


def solution(mesh):
    return jax.shard_map(
        functools.partial(local, mesh.shape["grp"], mesh.shape["rep"]),
        mesh=mesh,
        in_specs=(P(("grp", "rep"), None), P(("grp", "rep"), None), P()),
        out_specs=(P(), P(("grp", "rep"), None)),
        check_vma=False,
    )
```

```python
import math

import functools

import jax
import jax.numpy as jnp
import numpy as np
from jax import lax
from jax.experimental import pallas as pl
from jax.experimental.pallas import tpu as pltpu
from jax.sharding import PartitionSpec as P

BLOCK = 64
TOPK = 32
CH_OWN = 1


def dct_cosines(points):
    freq = jnp.arange(points, dtype=jnp.float32)[:, None]
    place = jnp.arange(points, dtype=jnp.float32)[None, :]
    values = jnp.cos(jnp.pi * (2.0 * place + 1.0) * freq / (2.0 * points)) * jnp.sqrt(2.0 / points)
    values = values.at[0].multiply(jnp.sqrt(0.5))
    rounded = lax.optimization_barrier(values.astype(jnp.bfloat16))
    return rounded.astype(jnp.float32)


def forward(square_low, cosines, cos_low):
    half = jnp.einsum("cab,jb->caj", square_low, cos_low, preferred_element_type=jnp.float32)
    return jnp.einsum("ia,caj->cij", cosines, half, precision=lax.Precision.HIGHEST)


def decode(dense_matrix, cosines):
    square = dense_matrix.reshape(dense_matrix.shape[0], BLOCK, BLOCK)
    half = jnp.einsum("cij,jb->cib", square, cosines, precision=lax.Precision.HIGHEST)
    full = jnp.einsum("ia,cib->cab", cosines, half, precision=lax.Precision.HIGHEST)
    return full.reshape(dense_matrix.shape[0], BLOCK * BLOCK)


def decode_sparse(dense_low, cosines, cos_low):
    square = dense_low.reshape(dense_low.shape[0], BLOCK, BLOCK)
    half = jnp.einsum("cij,jb->cib", square, cos_low, preferred_element_type=jnp.float32)
    full = jnp.einsum("ia,cib->cab", cosines, half, precision=lax.Precision.HIGHEST)
    return full.reshape(dense_low.shape[0], BLOCK * BLOCK)


def densify(values, spots):
    entries, columns = values.shape
    per_step = math.gcd(entries, max(1, 65536 // columns))
    positions = jnp.arange(BLOCK, dtype=jnp.int32)

    def one_block(pieces):
        block_values, block_spots = pieces
        zeros = jnp.zeros_like(block_values)
        row_onehot = jnp.where(
            (block_spots // BLOCK)[:, None, :] == positions[None, :, None],
            block_values[:, None, :],
            zeros[:, None, :],
        )
        column_onehot = ((block_spots % BLOCK)[:, None, :] == positions[None, :, None]).astype(
            jnp.bfloat16
        )
        dense_matrix = jnp.einsum(
            "bcy,bzy->bcz", row_onehot, column_onehot, preferred_element_type=jnp.float32
        )
        return dense_matrix.reshape(per_step, BLOCK * BLOCK)

    stacked = lax.map(
        one_block,
        (
            values.reshape(entries // per_step, per_step, columns),
            spots.reshape(entries // per_step, per_step, columns),
        ),
    )
    return stacked.reshape(entries, BLOCK * BLOCK)


def owner_sum(received):
    values, spots = received
    return densify(values[0], spots[0])


def local_large(momentum, picked, owner_span_order):
    cosines = dct_cosines(BLOCK)
    cos_low = cosines.astype(jnp.bfloat16)
    owners = lax.axis_size("grp")
    span_count = momentum.shape[0]
    square_low = momentum.reshape(span_count, BLOCK, BLOCK)
    transform_coefficients = forward(square_low, cosines, cos_low).reshape(
        span_count, BLOCK * BLOCK
    )
    chosen = jnp.take_along_axis(transform_coefficients, picked, axis=1).astype(jnp.bfloat16)
    own_dense = densify(chosen, picked).astype(jnp.bfloat16)
    residual_momentum = (
        momentum.astype(jnp.float32) - decode_sparse(own_dense, cosines, cos_low)
    ).astype(jnp.bfloat16)
    slot_values = jnp.take(chosen, owner_span_order, axis=0)
    slot_spots = jnp.take(picked, owner_span_order, axis=0)
    shaped = (slot_values.reshape(owners, CH_OWN, TOPK), slot_spots.reshape(owners, CH_OWN, TOPK))
    partial_sum = owner_sum(
        (
            lax.all_to_all(shaped[0], "grp", split_axis=0, concat_axis=2, tiled=True),
            lax.all_to_all(shaped[1], "grp", split_axis=0, concat_axis=2, tiled=True),
        )
    )
    partial_sum = lax.psum(partial_sum, "rep")
    my_share = decode(partial_sum, cosines).astype(jnp.bfloat16)
    update = lax.all_gather(my_share, "grp", axis=0, tiled=True)
    return (update, residual_momentum)


LANES = 128
GATHER_BYTES = 2**20


def cosine_table():
    freq = np.arange(BLOCK, dtype=np.float64)[:, None]
    place = np.arange(BLOCK, dtype=np.float64)[None, :]
    values = np.cos(np.pi * (2 * place + 1) * freq / (2 * BLOCK)) * np.sqrt(2 / BLOCK)
    values[0] *= np.sqrt(0.5)
    return values.astype(np.float32)


def contract_lanes(left, right):
    return lax.dot_general(
        left, right, (((1,), (1,)), ((), ())), preferred_element_type=jnp.float32
    )


def matmul(left, right):
    return jnp.dot(left, right, preferred_element_type=jnp.float32)


def split(value):
    high = value.astype(jnp.bfloat16)
    return high, (value - high.astype(jnp.float32)).astype(jnp.bfloat16)


def exchange_kernel(
    groups,
    planes,
    order_hbm,
    momentum_hbm,
    picked_hbm,
    rows_hbm,
    cols_hbm,
    twice_hbm,
    pairs_hbm,
    update_ref,
    residual_ref,
    order_ref,
    momentum_ref,
    picked_ref,
    rows_ref,
    cols_ref,
    twice_ref,
    pairs_ref,
    box,
    turned,
    dense,
    decoded,
    load_sem,
    send_sem,
    recv_sem,
):
    sources = (picked_hbm, cols_hbm, rows_hbm, momentum_hbm, twice_hbm, pairs_hbm, order_hbm)
    targets = (picked_ref, cols_ref, rows_ref, momentum_ref, twice_ref, pairs_ref, order_ref)
    loads = [
        pltpu.make_async_copy(source, target, load_sem.at[n])
        for n, (source, target) in enumerate(zip(sources, targets))
    ]
    for load in loads:
        load.start()
    spans = momentum_ref.shape[0]
    entries = spans * TOPK
    chunks = BLOCK * BLOCK // LANES
    in_tile = LANES // TOPK
    tiles = entries // LANES
    devices = groups * planes
    my_group, my_plane = lax.axis_index("grp"), lax.axis_index("rep")
    group_of = [lax.rem(my_group + step, groups) for step in range(groups)]
    plane_of = [lax.rem(my_plane + step, planes) for step in range(planes)]

    def peer(plane, group):
        return {"grp": group_of[group], "rep": plane_of[plane]}

    others = [(z, g) for z in range(planes) for g in range(groups) if z or g]
    far_first = [o for o in others if o[0]] + [o for o in others if not o[0]]
    barrier = pltpu.get_barrier_semaphore()
    for z, g in far_first:
        pl.semaphore_signal(barrier, inc=1, device_id=peer(z, g), device_id_type=pl.DeviceIdType.MESH)

    loads[0].wait()
    lane = lax.broadcasted_iota(jnp.int32, (spans, entries), 1)
    mine = (lane // TOPK) == lax.broadcasted_iota(jnp.int32, (spans, entries), 0)
    spread = jnp.concatenate([picked_ref[...]] * spans, axis=1)
    spots = jnp.sum(jnp.where(mine, spread, 0), axis=0, keepdims=True)
    freq = lax.broadcasted_iota(jnp.int32, (BLOCK, entries), 0)
    row_spot, col_spot = spots // BLOCK, spots % BLOCK
    one_row = jnp.where(freq == row_spot, 1.0, 0.0).astype(jnp.bfloat16)
    one_col = jnp.where(freq == col_spot, 1.0, 0.0).astype(jnp.bfloat16)
    half_rows = chunks * spans
    for load in loads[1:]:
        load.wait()
    wave = matmul(cols_ref[...], one_col).astype(jnp.bfloat16)
    blank = jnp.zeros_like(wave)
    waves = (jnp.concatenate([wave, blank], axis=0), jnp.concatenate([blank, wave], axis=0))
    momentum = jnp.concatenate(
        [momentum_ref[:, k * LANES : (k + 1) * LANES].astype(jnp.float32) for k in range(chunks)],
        axis=0,
    )
    momentum_low = momentum.astype(jnp.bfloat16)
    total = jnp.zeros((spans, entries), jnp.float32)
    row_waves = []
    for p in range(2):
        row_wave = matmul(rows_ref[p * half_rows : (p + 1) * half_rows, :], one_row)
        row_waves.append(row_wave)
        product = row_wave * matmul(momentum_low, waves[p])
        total += jnp.sum(product.reshape(chunks, spans, entries), axis=0)
    chosen = jnp.sum(jnp.where(mine, total, 0.0), axis=0, keepdims=True)
    chosen_low = chosen.astype(jnp.bfloat16)
    chosen = chosen_low.astype(jnp.float32)

    def by_tile(row):
        return jnp.concatenate(
            [row[:, h * LANES : (h + 1) * LANES] for h in range(tiles)], axis=0
        )

    def store_residual():
        correction = jnp.zeros((half_rows, LANES), jnp.float32)
        scaled = jnp.where(mine, chosen, 0.0)
        for p in range(2):
            weight = row_waves[p].reshape(chunks, spans, entries) * scaled[None]
            for part in split(weight.reshape(half_rows, entries)):
                correction += contract_lanes(part, waves[p])
        residual = momentum - correction
        for k in range(chunks):
            residual_ref[:, k * LANES : (k + 1) * LANES] = residual[
                k * spans : (k + 1) * spans
            ].astype(jnp.bfloat16)

    parts = [by_tile(part) for part in (chosen, row_spot.astype(jnp.float32), col_spot.astype(jnp.float32))]
    for turn in range(in_tile):
        turned[turn] = jnp.concatenate(
            [pltpu.roll(part, turn * TOPK, 1).astype(jnp.bfloat16) for part in parts], axis=1
        )
    box[0] = jnp.concatenate([part.astype(jnp.bfloat16) for part in parts], axis=1)
    pl.when(my_plane == 0)(store_residual)
    pl.semaphore_wait(barrier, devices - 1)
    copies = []
    for z, g in far_first:
        copy = pltpu.make_async_remote_copy(
            src_ref=turned.at[g % in_tile],
            dst_ref=box.at[z * groups + g],
            send_sem=send_sem,
            recv_sem=recv_sem.at[z],
            device_id=peer(z, g),
            device_id_type=pl.DeviceIdType.MESH,
        )
        copy.start()
        copies.append(copy)

    block = lax.broadcasted_iota(jnp.int32, (tiles, LANES), 1) // TOPK
    taken = [block == turn for turn in range(in_tile)]
    freq = lax.broadcasted_iota(jnp.int32, (BLOCK, groups * TOPK), 0)
    freq = freq.astype(jnp.float32).astype(jnp.bfloat16)
    one, zero = jnp.ones((), jnp.bfloat16), jnp.zeros((), jnp.bfloat16)

    def span_rows(rows, c):
        picks = []
        for first in range(0, groups, in_tile):
            row = rows[first]
            for turn in range(1, in_tile):
                row = jnp.where(taken[(c + turn) % in_tile], rows[first + turn], row)
            picks.append(row)
        return jnp.concatenate(picks, axis=1)

    sums = [None] * spans
    for z in range(planes):
        first = 1 if z == 0 else 0
        landed = box.at[pl.ds(z * groups + first, groups - first)]
        pltpu.make_async_copy(landed, landed, recv_sem.at[z]).wait()
        slots = [box[z * groups + g].astype(jnp.float32) for g in range(groups)]
        values, rows, columns = (
            [slot[:, n * LANES : (n + 1) * LANES] for slot in slots] for n in range(3)
        )
        for c in range(in_tile):
            value, row, column = (
                span_rows(part, c).astype(jnp.bfloat16) for part in (values, rows, columns)
            )
            for h in range(tiles):
                left = jnp.where(freq == row[h : h + 1], one, zero)
                right = jnp.where(freq == column[h : h + 1], value[h : h + 1], zero)
                part = contract_lanes(left, right)
                span = h * in_tile + c
                sums[span] = part if z == 0 else sums[span] + part
    for span in range(spans):
        dense[span] = matmul(sums[span].astype(jnp.bfloat16), twice_ref[...])
    lower = lax.broadcasted_iota(jnp.int32, (chunks, LANES), 1) < BLOCK
    for s in range(spans):
        full = matmul(pairs_ref[...], dense[order_ref[s]].astype(jnp.bfloat16))
        decoded[pl.ds(s, chunks, stride=spans), :] = jnp.where(
            lower, full[:chunks], full[chunks:]
        )
    for k in range(chunks):
        update_ref[:, k * LANES : (k + 1) * LANES] = decoded[
            k * spans : (k + 1) * spans, :
        ].astype(jnp.bfloat16)
    pl.when(my_plane != 0)(store_residual)
    for copy in copies:
        copy.wait_send()


def store_kernel(update_ref, residual_ref, update_hbm, residual_hbm, sem):
    stores = [
        pltpu.make_async_copy(residual_ref, residual_hbm, sem.at[0]),
        pltpu.make_async_copy(update_ref, update_hbm, sem.at[1]),
    ]
    for store in stores:
        store.start()
    for store in stores:
        store.wait()


def local_small(groups, planes, momentum, picked, owner_span_order):
    spans = momentum.shape[0]
    chunks = BLOCK * BLOCK // LANES
    table = cosine_table()
    by_pair = table.T.reshape(chunks, 2, BLOCK)
    rows = np.repeat(by_pair.transpose(1, 0, 2), spans, axis=1).reshape(-1, BLOCK)
    constants = [rows, table.T, np.concatenate([table, table], axis=1), by_pair.transpose(1, 0, 2).reshape(-1, BLOCK)]
    constants = [jnp.asarray(constant, dtype=jnp.bfloat16) for constant in constants]
    operands = [owner_span_order, momentum, picked, *constants]
    anywhere = pl.BlockSpec(memory_space=pl.ANY)
    vmem = pl.BlockSpec(memory_space=pltpu.VMEM)
    devices = groups * planes
    tile_shape = (spans * TOPK // LANES, 3 * LANES)
    results = pl.pallas_call(
        functools.partial(exchange_kernel, groups, planes),
        out_shape=[pltpu.VMEM(momentum.shape, jnp.bfloat16)] * 2,
        in_specs=[anywhere] * len(operands),
        out_specs=[vmem] * 2,
        scratch_shapes=[pltpu.SMEM(owner_span_order.shape, jnp.int32)]
        + [pltpu.VMEM(x.shape, x.dtype) for x in operands[1:]]
        + [
            pltpu.VMEM((devices, *tile_shape), jnp.bfloat16),
            pltpu.VMEM((LANES // TOPK, *tile_shape), jnp.bfloat16),
            pltpu.VMEM((spans, BLOCK, LANES), jnp.float32),
            pltpu.VMEM((chunks * spans, LANES), jnp.float32),
            pltpu.SemaphoreType.DMA((len(operands),)),
            pltpu.SemaphoreType.DMA,
            pltpu.SemaphoreType.DMA((planes,)),
        ],
        compiler_params=pltpu.CompilerParams(collective_id=0, has_side_effects=True),
    )(*operands)
    return pl.pallas_call(
        store_kernel,
        out_shape=[jax.ShapeDtypeStruct(momentum.shape, jnp.bfloat16)] * 2,
        in_specs=[vmem] * 2,
        out_specs=[anywhere] * 2,
        scratch_shapes=[pltpu.SemaphoreType.DMA((2,))],
    )(*[pltpu.with_memory_space_constraint(result, pltpu.VMEM) for result in results])


def local(groups, planes, momentum, picked, owner_span_order):
    entries = momentum.shape[0] * TOPK
    if entries % LANES == 0 and groups % (LANES // TOPK) == 0 and groups * planes * entries * 8 <= GATHER_BYTES:
        return local_small(groups, planes, momentum, picked, owner_span_order)
    return local_large(momentum, picked, owner_span_order)


def solution(mesh):
    return jax.shard_map(
        functools.partial(local, mesh.shape["grp"], mesh.shape["rep"]),
        mesh=mesh,
        in_specs=(P(("grp", "rep"), None), P(("grp", "rep"), None), P()),
        out_specs=(P(), P(("grp", "rep"), None)),
        check_vma=False,
    )
```
